32 devices in a mesh: dp: 8 (over z, y), mp: 4 (over x, core).
Axes of the slice: x: 2, y: 2, z: 4, core: 2. Of those that a mesh axis runs over, the one named last changes fastest.
Arguments:
- frames: int32 [48], P('dp'), may hold values from 17 to 129, as said below
- owners: int32 [240], P('dp'), may hold values from -1 to 7, as said below
- offsets: int32 [240], P('dp'), may hold values from -1 to 17, as said below
- groups: int32 [48], P('dp'), may hold values from 0 to 3, as said below
- latent: bfloat16 [240, 64, 128], P('dp'), may hold values from -12 to 12
- noise_blocks: bfloat16 [240, 64, 128], P('dp'), may hold values from -6 to 6
- rewards: float32 [48], P('dp'), may hold values from -6 to 6
- embed_weight: bfloat16 [64, 3072], replicated, may hold values from -2 to 2
- norm_gain: float32 [3072], replicated, may hold values from 0 to 2
- mid_weight: bfloat16 [3072, 3072], P(None, 'mp'), may hold values from -1 to 1
- head_weight: bfloat16 [3072, 64], P('mp'), may hold values from -1 to 1
Outputs:
- prediction: bfloat16 [144, 64, 128], P('dp')
- log_prob: float32 [48], P('dp')
- advantage: float32 [48], P('dp')
The draws below stay inside these ranges and needn't reach their ends.
Inputs may be any that keep to these rules, and one draw needn't show every extreme that they name: frames = 4 m + 1 for a whole m; the block counts (frames - 1) // 32 + 1 of all samples add up to exactly 144, and some rollout device has all its samples at 129 frames. `owners`: a live slot names its owner, an empty one -1; every owner receives exactly 18 blocks; one rollout device sends at most 4 blocks to one owner, and in every draw some device sends that many to some owner. `offsets`: a live slot's row at its owner, rows distinct at each owner; empty slots -1. `groups`: every prompt has exactly 12 samples.
All inputs are finite; a program needn't handle non-finite values.
Results may differ from the reference program's by a relative error of at most 0.0068.
Values may be sent and summed in bfloat16 or wider, within the bound.
A program may use at most 64 MiB of HBM per device.

```python
import math
import jax
import jax.numpy as jnp
from jax import lax

D = 3072
C = 64
BT = 128
MAXB = 5
GSIZE = 12
SPD = 6
SAMPLES = 48
GROUPS = 4
OB = 18
N_DP = 8


def layout(key):
    devices = SAMPLES // SPD
    half_dev = devices // 2
    bias_key = jax.random.fold_in(key, 101)
    shift_key = jax.random.fold_in(key, 102)
    force_key = jax.random.fold_in(key, 103)
    sides_key = jax.random.fold_in(key, 104)
    frame_key = jax.random.fold_in(key, 105)
    order_key = jax.random.fold_in(key, 106)
    device_bias = jax.random.randint(bias_key, (half_dev, 1), -1, 2)
    shifts = jnp.clip(device_bias + jax.random.randint(shift_key, (half_dev, SPD), -1, 2), -2, 2)
    forced = jax.random.randint(force_key, (), 0, half_dev)
    shifts = jnp.where(jnp.arange(half_dev)[:, None] == forced, 2, shifts)
    sides = jax.random.randint(sides_key, (half_dev, 1), 0, 2)
    first_counts = jnp.where(sides == 0, 3 + shifts, 3 - shifts)
    counts = jnp.concatenate([first_counts, 6 - first_counts], axis=0)
    extra_frames = jax.random.randint(frame_key, (devices, SPD), 0, 8)
    latent_minus = jnp.where(counts == 1, jnp.maximum(extra_frames, 4), jnp.where(counts == 5, 32, 8 * (counts - 1) + extra_frames))
    frames = (4 * latent_minus + 1).reshape(-1).astype(jnp.int32)
    live_slot = (jnp.arange(MAXB)[None, None, :] < counts[:, :, None]).astype(jnp.int32)
    live_slot = live_slot.reshape(devices, SPD * MAXB)
    per_dev = jnp.sum(live_slot, axis=1)
    before = jnp.cumsum(per_dev) - per_dev
    within = jnp.cumsum(live_slot, axis=1) - 1
    global_rank = before[:, None] + within
    owner_order = jax.random.permutation(order_key, devices)
    owners = jnp.where(live_slot == 1, jnp.take(owner_order, global_rank % devices), -1)
    offsets = jnp.where(live_slot == 1, global_rank // devices, -1)
    return (frames, owners.reshape(-1).astype(jnp.int32), offsets.reshape(-1).astype(jnp.int32))


def draw_frames(key, part):
    return layout(key)[0]


def draw_owners(key, part):
    return layout(key)[1]


def draw_offsets(key, part):
    return layout(key)[2]


def draw_groups(key, part):
    return (jax.random.permutation(jax.random.fold_in(key, 7), SAMPLES) // GSIZE).astype(jnp.int32)


def base_values(key, shape, bound):
    return jnp.clip(jax.random.normal(key, shape, jnp.float32), -bound, bound)


def model_weights(key):
    embed = base_values(jax.random.fold_in(key, 201), (C, D), 6.0) / math.sqrt(C)
    gain = 1.0 + 0.15 * base_values(jax.random.fold_in(key, 202), (D,), 3.0)
    middle = base_values(jax.random.fold_in(key, 203), (D, D), 6.0) / math.sqrt(D)
    output = base_values(jax.random.fold_in(key, 204), (D, C), 6.0) / math.sqrt(D)
    return (embed, gain, middle, output)


def latent_values(key):
    raw = base_values(jax.random.fold_in(key, 205), (SAMPLES * MAXB, C, BT), 6.0)
    return raw


def rounded(values):
    narrow = lax.optimization_barrier(values.astype(jnp.bfloat16))
    return narrow.astype(jnp.float32)


def draw_latent(key, part):
    return latent_values(key).astype(jnp.bfloat16)


def draw_embed_weight(key, part):
    return model_weights(key)[0].astype(jnp.bfloat16)


def draw_norm_gain(key, part):
    return model_weights(key)[1].astype(jnp.float32)


def draw_mid_weight(key, part):
    return model_weights(key)[2].astype(jnp.bfloat16)


def draw_head_weight(key, part):
    return model_weights(key)[3].astype(jnp.bfloat16)


def draw_noise_blocks(key, part):
    embed, gain, middle, output = model_weights(key)
    embed = rounded(embed)
    middle = rounded(middle)
    output = rounded(output)
    latent = rounded(latent_values(key))

    def one_slot(block):
        embedded = jnp.dot(block.T, embed)
        mean_sq = jnp.mean(embedded * embedded, axis=-1, keepdims=True)
        normed = rounded(embedded / jnp.sqrt(mean_sq + 0.25) * gain)
        activated = rounded(jax.nn.silu(jnp.dot(normed, middle)))
        return jnp.dot(activated, output).T
    velocity = lax.map(one_slot, latent)
    sigma = jnp.exp(jax.random.uniform(jax.random.fold_in(key, 207), (SAMPLES * MAXB, 1, 1), jnp.float32, math.log(0.15), math.log(0.6)))
    fresh = base_values(jax.random.fold_in(key, 208), (SAMPLES * MAXB, C, BT), 6.0)
    return jnp.clip(sigma * fresh - velocity, -6.0, 6.0).astype(jnp.bfloat16)


def levels(rng, shape, split, least, largest):
    level, own = 1.0, jax.random.fold_in(rng, 6)
    for dim, blocks in split:
        heights = jnp.exp(jax.random.uniform(jax.random.fold_in(own, dim), (blocks,), jnp.float32, least / len(split), largest / len(split)))
        level = level * jnp.repeat(heights, shape[dim] // blocks).reshape([-1 if axis == dim else 1 for axis in range(len(shape))])
    return level


def scatter_about(stream_key, extent, spread, limit, shards=(), kind=jnp.bfloat16):
    level = levels(stream_key, extent, shards, -0.22, 0.18) if shards else 1.0
    entries = jax.random.normal(stream_key, extent, jnp.float32) * spread * level
    return jnp.minimum(jnp.maximum(entries, -limit), limit).astype(kind)


def setup_inputs(seed: int = 0) -> dict:
    key_of = jax.random.split(jax.random.key(seed), 12)
    frames = draw_frames(jax.random.fold_in(key_of[11], 71), 0)
    owners = draw_owners(jax.random.fold_in(key_of[11], 71), 0)
    offsets = draw_offsets(jax.random.fold_in(key_of[11], 71), 0)
    groups = draw_groups(jax.random.fold_in(key_of[11], 71), 0)
    latent = draw_latent(jax.random.fold_in(key_of[11], 71), 0)
    noise_blocks = draw_noise_blocks(jax.random.fold_in(key_of[11], 71), 0)
    rewards = scatter_about(key_of[6], (SAMPLES,), 1.0, 6.0, ((0, 8),), jnp.float32)
    embed_weight = draw_embed_weight(jax.random.fold_in(key_of[11], 71), 0)
    norm_gain = draw_norm_gain(jax.random.fold_in(key_of[11], 71), 0)
    mid_weight = draw_mid_weight(jax.random.fold_in(key_of[11], 71), 0)
    head_weight = draw_head_weight(jax.random.fold_in(key_of[11], 71), 0)
    return {"frames": frames, "owners": owners, "offsets": offsets, "groups": groups, "latent": latent, "noise_blocks": noise_blocks, "rewards": rewards, "embed_weight": embed_weight, "norm_gain": norm_gain, "mid_weight": mid_weight, "head_weight": head_weight}


def forward(latent_part, noise_part, embed_weight, norm_gain, mid_weight, head_weight):
    embedded = jnp.einsum('nct,cd->ntd', latent_part.astype(jnp.float32), embed_weight.astype(jnp.float32))
    mean_sq = lax.optimization_barrier(jnp.mean(embedded * embedded, axis=-1, keepdims=True))
    normed = (embedded * lax.rsqrt(mean_sq + 0.25) * norm_gain).astype(jnp.bfloat16)
    mid_out = jnp.einsum('ntd,df->ntf', normed.astype(jnp.float32), mid_weight.astype(jnp.float32))
    activated = jax.nn.silu(mid_out).astype(jnp.bfloat16)
    velocity = jnp.einsum('ntf,fc->nct', activated.astype(jnp.float32), head_weight.astype(jnp.float32))
    errors = noise_part.astype(jnp.float32) + velocity
    return (velocity.astype(jnp.bfloat16), lax.optimization_barrier(jnp.sum(errors * errors, axis=(1, 2))))

def reference(frames, owners, offsets, groups, latent, noise_blocks, rewards, embed_weight, norm_gain, mid_weight, head_weight):
    counts = ((frames - 1) // 32 + 1).astype(jnp.int32)
    slot_index = jnp.arange(SAMPLES * MAXB, dtype=jnp.int32)
    live_slot = slot_index % MAXB < jnp.repeat(counts, MAXB)
    dest_row = jnp.where(live_slot, owners * OB + offsets, N_DP * OB).astype(jnp.int32)
    owner_latent = jnp.zeros((N_DP * OB, C, BT), jnp.bfloat16).at[dest_row].set(latent, mode='drop')
    owner_noise = jnp.zeros((N_DP * OB, C, BT), jnp.bfloat16).at[dest_row].set(noise_blocks, mode='drop')
    sample_ids = (slot_index // MAXB).astype(jnp.int32)
    owner_sample = jnp.zeros((N_DP * OB,), jnp.int32).at[dest_row].set(sample_ids, mode='drop')

    def per_owner(pieces):
        return forward(pieces[0], pieces[1], embed_weight, norm_gain, mid_weight, head_weight)
    preds, slot_sums = lax.map(per_owner, (owner_latent.reshape(N_DP, OB, C, BT), owner_noise.reshape(N_DP, OB, C, BT)))
    prediction = preds.reshape(N_DP * OB, C, BT)
    totals = jax.ops.segment_sum(slot_sums.reshape(-1), owner_sample, num_segments=SAMPLES)
    log_prob = -0.5 * totals / (counts * BT * C).astype(jnp.float32)
    group_sum = jax.ops.segment_sum(rewards, groups, num_segments=GROUPS)
    group_sq = jax.ops.segment_sum(rewards * rewards, groups, num_segments=GROUPS)
    group_mean = group_sum / GSIZE
    variance = group_sq / GSIZE - group_mean * group_mean
    advantage = (rewards - group_mean[groups]) / jnp.sqrt(variance[groups] + 0.25)
    return (prediction, log_prob, advantage)
```

```python
import functools

import jax
import jax.numpy as jnp
from jax import lax
from jax.experimental import pallas as pl
from jax.experimental.pallas import tpu as pltpu
from jax.sharding import PartitionSpec as P

MAXB = 5
GSIZE = 12
F32 = jnp.float32
BF16 = jnp.bfloat16


def index_kernel(
    dims, frames, owners, offsets, groups, rewards, slots, info, count, row_of
):
    devices, cap, jm, bpc = dims
    for o in range(devices):
        count[o] = 0
    for i in range(devices * cap):
        slots[i] = -1
        row_of[i] = -1

    def place(i, z):
        live = i % MAXB < lax.shift_right_arithmetic(frames[i // MAXB] - 1, 5) + 1

        @pl.when(live)
        def _():
            o = owners[i]
            p = count[o]
            count[o] = p + 1
            slots[o * cap + p] = i
            row_of[o * cap + p] = offsets[i]

        return z

    lax.fori_loop(0, owners.shape[0], place, 0)
    row = lax.broadcasted_iota(jnp.int32, (8, 128), 0)
    lane = lax.broadcasted_iota(jnp.int32, (8, 128), 1)
    common = jnp.zeros((8, 128), F32)
    for i in range(frames.shape[0]):
        common = jnp.where((row == 1) & (lane == i), rewards[i], common)
        common = jnp.where((row == 2) & (lane == i), groups[i].astype(F32), common)

    def tile(o, z):
        t = common
        for j in range(cap):
            t = jnp.where((row == 0) & (lane == j), row_of[o * cap + j].astype(F32), t)
        info[o] = t
        return z

    lax.fori_loop(0, devices, tile, 0)


def main_kernel(
    dims, width, slots, embed, gain, head, info, latent, noise, mid,
    blocks, infos, errs,
    lat, noi, mids, tokens, wown, wbuf, wt, half, vel, pred, err, ebuf,
    wsend, wrecv, isend, irecv, psend, precv, gsend, grecv, esend, erecv, local_sem, load_sem,
):
    devices, cap, jm, bpc = dims
    c = embed.shape[0]
    bt = latent.shape[2]
    nchunk = tokens.shape[0]
    steps, kc, _ = mids.shape
    loads = [pltpu.make_async_copy(latent, lat, load_sem.at[0])]
    for i in range(steps):
        loads.append(
            pltpu.make_async_copy(mid.at[pl.ds(i * kc, kc)], mids.at[i], load_sem.at[1 + i])
        )
    loads.append(pltpu.make_async_copy(noise, noi, load_sem.at[1 + steps]))
    for cp in loads:
        cp.start()
    me = lax.axis_index("dp")
    m = lax.axis_index("mp")
    partner = m + 1 - 2 * (m % 2)
    across = (m + 2) % 4
    diag = (partner + 2) % 4

    def copy(src, dst, ssem, rsem, dp, mp):
        return pltpu.make_async_remote_copy(
            src_ref=src, dst_ref=dst, send_sem=ssem, recv_sem=rsem,
            device_id=(dp, mp), device_id_type=pl.DeviceIdType.MESH,
        )

    barrier = pltpu.get_barrier_semaphore()
    for p in (partner, across, diag):
        pl.semaphore_signal(
            barrier, inc=1, device_id=(me, p), device_id_type=pl.DeviceIdType.MESH
        )
    for d in range(1, devices):
        pl.semaphore_signal(
            barrier, inc=1, device_id=((me + d) % devices, m),
            device_id_type=pl.DeviceIdType.MESH,
        )
    w = embed[...]
    gram = lax.dot_general(w, w, (((1,), (1,)), ((), ())), preferred_element_type=F32)
    pl.semaphore_wait(barrier, 3 + devices - 1)

    def trio(src, part):
        return [
            copy(src, wbuf.at[0, part], wsend.at[0, part], wrecv.at[0, part], me, partner),
            copy(src, wbuf.at[1, part], wsend.at[1, part], wrecv.at[1, part], me, across),
            copy(
                wbuf.at[1, part], wbuf.at[2, part], wsend.at[2, part], wrecv.at[2, part],
                me, partner,
            ),
        ]

    hc = trio(head, 1)
    wc = trio(wown, 0)
    hc[1].start()
    hc[0].start()
    ic = [None]
    for d in range(1, devices):
        peer = (me + d) % devices
        cp = copy(info.at[peer], infos.at[me], isend.at[d], irecv.at[d], peer, m)
        cp.start()
        ic.append(cp)
    own_info = pltpu.make_async_copy(info.at[me], infos.at[me], local_sem.at[0])
    own_info.start()

    loads[0].wait()

    def prepare(k, z):
        for b in range(bpc):
            q = k * bpc + b
            s = jnp.maximum(slots[(q // jm) * cap + m * jm + q % jm], 0)
            tokens[k, :, b * bt : (b + 1) * bt] = lat[s]
        x = tokens[k].astype(F32)
        y = jnp.dot(gram, x, preferred_element_type=F32, precision=lax.Precision.HIGHEST)
        ms = jnp.maximum(jnp.sum(x * y, axis=0, keepdims=True), 0.0) / width
        half[k] = 0.5 * lax.rsqrt(ms + 0.25)
        return z

    lax.fori_loop(0, nchunk, prepare, 0)

    folded = None
    for i in range(steps):
        wg = embed[:, i * kc : (i + 1) * kc].astype(F32) * gain[:, i * kc : (i + 1) * kc]
        hi = wg.astype(BF16)
        lo = (wg - hi.astype(F32)).astype(BF16)
        loads[1 + i].wait()
        both = jnp.dot(
            jnp.concatenate([hi, lo], axis=0), mids[i], preferred_element_type=F32
        )
        folded = both if i == 0 else folded + both
    folded = folded[:c] + folded[c:]
    wown[...] = folded.astype(BF16)
    wt[...] = folded.T.astype(BF16)
    wc[1].start()
    wc[0].start()
    hc[1].wait_recv()
    hc[2].start()

    def part(href, k):
        u = jnp.dot(wt[...], tokens[k], preferred_element_type=F32)
        h = u * half[k]
        act = (h + h * jnp.tanh(h)).astype(BF16)
        return jnp.dot(href[...], act, preferred_element_type=F32)

    def share(href, first):
        def body(k, z):
            v = part(href, k)
            vel[k] = v if first else vel[k] + v
            return z

        lax.fori_loop(0, nchunk, body, 0)

    share(head, True)
    hc[0].wait_recv()
    wc[0].wait_recv()
    wt[...] = wbuf[0, 0].astype(F32).T.astype(BF16)
    share(wbuf.at[0, 1], False)
    wc[1].wait_recv()
    wc[2].start()
    wt[...] = wbuf[1, 0].astype(F32).T.astype(BF16)
    share(wbuf.at[1, 1], False)
    hc[2].wait_recv()
    wc[2].wait_recv()
    wt[...] = wbuf[2, 0].astype(F32).T.astype(BF16)
    err[...] = jnp.zeros_like(err)
    row = lax.broadcasted_iota(jnp.int32, err.shape, 0)
    loads[1 + steps].wait()

    def last(k, z):
        v = vel[k] + part(wbuf.at[2, 1], k)
        for b in range(bpc):
            q = k * bpc + b
            vb = v[:, b * bt : (b + 1) * bt]
            pred[q] = vb.astype(BF16)
            s = slots[(q // jm) * cap + m * jm + q % jm]
            e = noi[jnp.maximum(s, 0)].astype(F32) + vb
            e = jnp.sum(e * e, axis=0, keepdims=True)
            sample = jnp.where(s < 0, -1, s // MAXB)
            err[...] += jnp.where(row == sample, e, 0.0)
        return z

    lax.fori_loop(0, nchunk, last, 0)

    pc = [None]
    for d in range(1, devices):
        peer = (me + d) % devices
        cp = copy(
            pred.at[pl.ds(peer * jm, jm)], blocks.at[m, me], psend.at[d], precv.at[d], peer, m
        )
        cp.start()
        pc.append(cp)
    own = pltpu.make_async_copy(pred.at[pl.ds(me * jm, jm)], blocks.at[m, me], local_sem.at[1])
    own.start()
    ec = []
    for i, p in enumerate((partner, across, diag)):
        cp = copy(err, ebuf.at[i], esend.at[i], erecv.at[i], me, p)
        cp.start()
        ec.append(cp)

    gc = []
    for d in range(devices):
        src = (me - d + devices) % devices
        if d == 0:
            own.wait()
        else:
            pc[d].wait_recv()
        a = copy(
            blocks.at[m, src], blocks.at[m, src], gsend.at[0, d], grecv.at[0, d], me, across
        )
        b = copy(
            blocks.at[m, src], blocks.at[m, src], gsend.at[1, d], grecv.at[1, d], me, partner
        )
        a.start()
        b.start()
        gc += [a, b]
    relay = []
    for d in range(devices):
        src = (me - d + devices) % devices
        gc[2 * d].wait_recv()
        r = copy(
            blocks.at[across, src], blocks.at[across, src],
            gsend.at[2, d], grecv.at[2, d], me, partner,
        )
        r.start()
        relay.append(r)
    for i in range(3):
        ec[i].wait_recv()
    errs[...] = err[...] + ebuf[0] + ebuf[1] + ebuf[2]
    own_info.wait()
    for d in range(1, devices):
        ic[d].wait()
        pc[d].wait_send()
    for d in range(devices):
        gc[2 * d].wait_send()
        gc[2 * d + 1].wait()
        relay[d].wait()
    for i in range(3):
        hc[i].wait_send()
        wc[i].wait_send()
        ec[i].wait_send()


def place_kernel(rows, blocks, out):
    def body(k, z):
        r = rows[k]

        @pl.when(r >= 0)
        def _():
            out[r] = blocks[k]

        return z

    lax.fori_loop(0, blocks.shape[0], body, 0)


def local(
    frames, owners, offsets, groups, latent, noise_blocks, rewards,
    embed_weight, norm_gain, mid_weight, head_weight,
):
    spd = frames.shape[0]
    devices = lax.axis_size("dp")
    mp = lax.axis_size("mp")
    nslot, c, bt = latent.shape
    width = embed_weight.shape[1]
    hidden = mid_weight.shape[1]
    pair_cap = (nslot + devices - 1) // devices
    jm = (pair_cap + mp - 1) // mp
    cap = jm * mp
    bpc = 2 if devices * jm % 2 == 0 else 1
    nchunk = devices * jm // bpc
    dims = (devices, cap, jm, bpc)
    rows8 = (spd + 7) // 8 * 8
    steps = 4
    kc = width // steps
    smem = pl.BlockSpec(memory_space=pltpu.SMEM)
    vmem = pl.BlockSpec(memory_space=pltpu.VMEM)
    hbm = pl.BlockSpec(memory_space=pl.ANY)
    shape = jax.ShapeDtypeStruct
    slots, info = pl.pallas_call(
        functools.partial(index_kernel, dims),
        in_specs=[smem] * 5,
        out_specs=[smem, vmem],
        out_shape=[shape((devices * cap,), jnp.int32), shape((devices, 8, 128), F32)],
        scratch_shapes=[
            pltpu.SMEM((devices,), jnp.int32),
            pltpu.SMEM((devices * cap,), jnp.int32),
        ],
        name="index",
    )(frames, owners, offsets, groups, rewards)
    dma = pltpu.SemaphoreType.DMA
    blocks, infos, errs = pl.pallas_call(
        functools.partial(main_kernel, dims, width),
        in_specs=[smem] + [vmem] * 4 + [hbm] * 3,
        out_specs=[vmem] * 3,
        out_shape=[
            shape((mp, devices, jm, c, bt), BF16),
            shape((devices, 8, 128), F32),
            shape((rows8, bt), F32),
        ],
        scratch_shapes=[
            pltpu.VMEM((nslot, c, bt), BF16),
            pltpu.VMEM((nslot, c, bt), BF16),
            pltpu.VMEM((steps, kc, hidden), BF16),
            pltpu.VMEM((nchunk, c, bpc * bt), BF16),
            pltpu.VMEM((c, hidden), BF16),
            pltpu.VMEM((3, 2, c, hidden), BF16),
            pltpu.VMEM((hidden, c), BF16),
            pltpu.VMEM((nchunk, 1, bpc * bt), F32),
            pltpu.VMEM((nchunk, c, bpc * bt), F32),
            pltpu.VMEM((devices * jm, c, bt), BF16),
            pltpu.VMEM((rows8, bt), F32),
            pltpu.VMEM((3, rows8, bt), F32),
            dma((3, 2)), dma((3, 2)),
            dma((devices,)), dma((devices,)),
            dma((devices,)), dma((devices,)),
            dma((3, devices)), dma((3, devices)),
            dma((3,)), dma((3,)),
            dma((2,)), dma((steps + 2,)),
        ],
        compiler_params=pltpu.CompilerParams(collective_id=0, has_side_effects=True),
        name="exchange",
    )(
        slots, embed_weight, norm_gain.reshape(1, width), head_weight.T, info,
        latent, noise_blocks, mid_weight,
    )
    where = infos[:, 0, :cap].reshape(devices, mp, jm).transpose(1, 0, 2).reshape(-1)
    prediction = pl.pallas_call(
        place_kernel,
        in_specs=[smem, vmem],
        out_specs=vmem,
        out_shape=shape((3 * spd, c, bt), BF16),
        name="place",
    )(where.astype(jnp.int32), blocks.reshape(mp * devices * jm, c, bt))
    counts = (frames - 1) // 32 + 1
    log_prob = -0.5 * jnp.sum(errs[:spd], axis=1) / (counts * bt * c).astype(F32)
    all_rewards = infos[:, 1, :spd].reshape(-1)
    same = groups.astype(F32)[:, None] == infos[:, 2, :spd].reshape(-1)[None, :]
    mean = jnp.sum(jnp.where(same, all_rewards[None, :], 0.0), axis=1) / GSIZE
    meansq = jnp.sum(jnp.where(same, (all_rewards * all_rewards)[None, :], 0.0), axis=1) / GSIZE
    advantage = (rewards - mean) / jnp.sqrt(meansq - mean * mean + 0.25)
    return (prediction, log_prob, advantage)


def solution(mesh):
    placed = (
        P("dp"),
        P("dp"),
        P("dp"),
        P("dp"),
        P("dp", None, None),
        P("dp", None, None),
        P("dp"),
        P(),
        P(),
        P(None, "mp"),
        P("mp", None),
    )
    return jax.shard_map(
        local,
        mesh=mesh,
        in_specs=placed,
        out_specs=(P("dp", None, None), P("dp"), P("dp")),
        check_vma=False,
    )
```

```python
import functools

import jax
import jax.numpy as jnp
from jax import lax
from jax.experimental import pallas as pl
from jax.experimental.pallas import tpu as pltpu
from jax.sharding import PartitionSpec as P

MAXB = 5
GSIZE = 12
F32 = jnp.float32
BF16 = jnp.bfloat16


def main_kernel(
    dims, frames, owners, offsets, groups, rewards, embed, gain, head, latent, noise, mid,
    out, fin,
    lat, noi, mids, tokens, wown, wbuf, wt, half, vel, pred, blocks, err, ebuf,
    slot_v, slot_s, ints, intr, flts, fltr, pos_v, pos_s,
    wsend, wrecv, isend, irecv, psend, precv, gsend, grecv, esend, erecv, local_sem, load_sem,
):
    devices, mp, jm, bpc = dims
    cap = jm * mp
    c, width = embed.shape
    bt = latent.shape[2]
    nslot = owners.shape[0]
    spd = frames.shape[0]
    nchunk = tokens.shape[0]
    nblk = devices * jm
    steps, kc, _ = mids.shape
    short = nchunk <= 4
    loads = [pltpu.make_async_copy(latent, lat, load_sem.at[0])]
    for i in range(steps):
        loads.append(
            pltpu.make_async_copy(mid.at[pl.ds(i * kc, kc)], mids.at[i], load_sem.at[1 + i])
        )
    loads.append(pltpu.make_async_copy(noise, noi, load_sem.at[1 + steps]))
    for cp in loads:
        cp.start()
    me = lax.axis_index("dp")
    m = lax.axis_index("mp")
    partner = m + 1 - 2 * (m % 2)
    across = (m + 2) % 4
    diag = (partner + 2) % 4

    def copy(src, dst, ssem, rsem, dp, mp):
        return pltpu.make_async_remote_copy(
            src_ref=src, dst_ref=dst, send_sem=ssem, recv_sem=rsem,
            device_id=(dp, mp), device_id_type=pl.DeviceIdType.MESH,
        )

    barrier = pltpu.get_barrier_semaphore()
    for p in (partner, across, diag):
        pl.semaphore_signal(
            barrier, inc=1, device_id=(me, p), device_id_type=pl.DeviceIdType.MESH
        )
    for d in range(1, devices):
        pl.semaphore_signal(
            barrier, inc=1, device_id=((me + d) % devices, m),
            device_id_type=pl.DeviceIdType.MESH,
        )

    row = lax.broadcasted_iota(jnp.int32, slot_v.shape, 0)
    lane = lax.broadcasted_iota(jnp.int32, slot_v.shape, 1)
    slot_of = jnp.full(slot_v.shape, -1, jnp.int32)
    row_of = slot_of
    seen = jnp.zeros(slot_v.shape, jnp.int32)
    live = jnp.ones((1, 128), jnp.int32)
    lane1 = lax.broadcasted_iota(jnp.int32, (1, 128), 1)
    for i in range(nslot):
        if i % MAXB == 0:
            blocks_here = lax.shift_right_arithmetic(frames[i // MAXB] - 1, 5) + 1
            live = jnp.where(lane1 == i // MAXB, blocks_here, live)
        hit = lane == jnp.where(i % MAXB < blocks_here, owners[i], -1)
        new = hit & (seen == row)
        slot_of = jnp.where(new, i, slot_of)
        row_of = jnp.where(new, offsets[i], row_of)
        seen = jnp.where(hit, seen + 1, seen)
    slot_v[...] = slot_of
    ints[...] = row_of
    frow = lax.broadcasted_iota(jnp.int32, (8, 128), 0)
    flane = lax.broadcasted_iota(jnp.int32, (8, 128), 1)
    table = jnp.full((8, 128), -1.0, F32)
    for i in range(spd):
        table = jnp.where((frow == 0) & (flane == i), rewards[i], table)
        table = jnp.where((frow == 1) & (flane == i), groups[i].astype(F32), table)
    flts[...] = table
    to_smem = pltpu.make_async_copy(slot_v, slot_s, local_sem.at[0])
    to_smem.start()
    w = embed[...]
    gram = lax.dot_general(w, w, (((1,), (1,)), ((), ())), preferred_element_type=F32)
    pl.semaphore_wait(barrier, 3 + devices - 1)

    def trio(src, part):
        return [
            copy(src, wbuf.at[0, part], wsend.at[0, part], wrecv.at[0, part], me, partner),
            copy(src, wbuf.at[1, part], wsend.at[1, part], wrecv.at[1, part], me, across),
            copy(
                wbuf.at[1, part], wbuf.at[2, part], wsend.at[2, part], wrecv.at[2, part],
                me, partner,
            ),
        ]

    hc = trio(head, 1)
    wc = trio(wown, 0)
    hc[1].start()
    hc[0].start()
    ic = []
    for d in range(1, devices):
        peer = (me + d) % devices
        ic.append(copy(ints, intr.at[me], isend.at[0, d], irecv.at[0, d], peer, m))
        ic.append(copy(flts, fltr.at[me], isend.at[1, d], irecv.at[1, d], peer, m))
    for cp in ic:
        cp.start()
    intr[me] = row_of
    fltr[me] = table

    to_smem.wait()
    loads[0].wait()

    def prepare(k, z):
        for b in range(bpc):
            q = k * bpc + b
            s = jnp.maximum(slot_s[m * jm + q % jm, q // jm], 0)
            tokens[k, :, b * bt : (b + 1) * bt] = lat[s]
        x = tokens[k].astype(F32)
        y = jnp.dot(gram, x, preferred_element_type=F32, precision=lax.Precision.HIGHEST)
        ms = jnp.maximum(jnp.sum(x * y, axis=0, keepdims=True), 0.0) / width
        half[k] = 0.5 * lax.rsqrt(ms + 0.25)
        return z

    lax.fori_loop(0, nchunk, prepare, 0, unroll=short)

    folded = None
    for i in range(steps):
        wg = embed[:, i * kc : (i + 1) * kc].astype(F32) * gain[:, i * kc : (i + 1) * kc]
        hi = wg.astype(BF16)
        lo = (wg - hi.astype(F32)).astype(BF16)
        loads[1 + i].wait()
        both = jnp.dot(
            jnp.concatenate([hi, lo], axis=0), mids[i], preferred_element_type=F32
        )
        folded = both if i == 0 else folded + both
    folded = folded[:c] + folded[c:]
    wown[...] = folded.astype(BF16)
    wt[...] = folded.T.astype(BF16)
    wc[1].start()
    wc[0].start()
    hc[1].wait_recv()
    hc[2].start()

    def part(href, k):
        u = jnp.dot(wt[...], tokens[k], preferred_element_type=F32)
        h = u * half[k]
        act = (h + h * jnp.tanh(h)).astype(BF16)
        return jnp.dot(href[...], act, preferred_element_type=F32)

    def share(href, first):
        def body(k, z):
            v = part(href, k)
            vel[k] = v if first else vel[k] + v
            return z

        lax.fori_loop(0, nchunk, body, 0, unroll=short)

    share(head, True)
    hc[0].wait_recv()
    wc[0].wait_recv()
    wt[...] = wbuf[0, 0].astype(F32).T.astype(BF16)
    share(wbuf.at[0, 1], False)
    wc[1].wait_recv()
    wc[2].start()
    wt[...] = wbuf[1, 0].astype(F32).T.astype(BF16)
    share(wbuf.at[1, 1], False)
    hc[2].wait_recv()
    wc[2].wait_recv()
    wt[...] = wbuf[2, 0].astype(F32).T.astype(BF16)
    err[...] = jnp.zeros_like(err)
    erow = lax.broadcasted_iota(jnp.int32, err.shape, 0)
    loads[1 + steps].wait()

    def sending(q):
        o, jj = q // jm, q % jm
        return copy(
            pred.at[q], blocks.at[(m * devices + me) * jm + jj],
            psend.at[q], precv.at[me * jm + jj], o, m,
        )

    def keeping(q):
        return pltpu.make_async_copy(
            pred.at[q], blocks.at[(m * devices + me) * jm + q % jm], psend.at[q]
        )

    def last(step, z):
        k = (me * jm // bpc + 1 + step) % nchunk
        v = vel[k] + part(wbuf.at[2, 1], k)
        for b in range(bpc):
            q = k * bpc + b
            vb = v[:, b * bt : (b + 1) * bt]
            pred[q] = vb.astype(BF16)

            @pl.when(q // jm != me)
            def _():
                sending(q).start()

            @pl.when(q // jm == me)
            def _():
                keeping(q).start()

            s = slot_s[m * jm + q % jm, q // jm]
            e = noi[jnp.maximum(s, 0)].astype(F32) + vb
            e = jnp.sum(e * e, axis=0, keepdims=True)
            sample = jnp.where(s < 0, -1, s // MAXB)
            err[...] += jnp.where(erow == sample, e, 0.0)
        return z

    lax.fori_loop(0, nchunk, last, 0, unroll=short)
    ec = []
    for i, p in enumerate((partner, across, diag)):
        cp = copy(err, ebuf.at[i], esend.at[i], erecv.at[i], me, p)
        cp.start()
        ec.append(cp)

    def moves(n, src, jj):
        at = blocks.at[(m * devices + src) * jm + jj]
        far = blocks.at[(across * devices + src) * jm + jj]
        return (
            copy(at, at, gsend.at[0, n], grecv.at[0, n], me, across),
            copy(at, at, gsend.at[1, n], grecv.at[1, n], me, partner),
            copy(far, far, gsend.at[2, n], grecv.at[2, n], me, partner),
        )

    gc = []
    for d in range(devices):
        src = (me - d + devices) % devices
        for jj in range(jm):
            trip = moves(d * jm + jj, src, jj)
            gc.append(trip)
            if d == 0:
                keeping(me * jm + jj).wait()
            else:
                pltpu.make_async_remote_copy(
                    src_ref=pred.at[0], dst_ref=blocks.at[(m * devices + src) * jm + jj],
                    send_sem=psend.at[0], recv_sem=precv.at[src * jm + jj],
                    device_id=(src, m), device_id_type=pl.DeviceIdType.MESH,
                ).wait_recv()
            trip[0].start()
            trip[1].start()
        if d == 0:
            for cp in ic:
                cp.wait_recv()
            code = jnp.full(slot_v.shape, -1, jnp.int32)
            for j in range(cap):
                code = jnp.where(row == j, (j // jm * devices) * jm + j % jm, code)
            pos = jnp.zeros(slot_v.shape, jnp.int32)
            mean = jnp.zeros((1, 128), F32)
            square = jnp.zeros((1, 128), F32)
            for s in range(devices):
                want = jnp.max(
                    jnp.where((lane == me) & (row < cap), intr[s], -1), axis=1, keepdims=True
                )
                pos = jnp.maximum(pos, jnp.where(want == lane, code + s * jm, 0))
            pos_v[...] = jnp.broadcast_to(jnp.max(pos, axis=0, keepdims=True), pos_v.shape)
            place = pltpu.make_async_copy(pos_v, pos_s, local_sem.at[1])
            place.start()
            every = fltr[:, 0, :]
            group = fltr[:, 1, :]
            for i in range(spd):
                mine = jnp.where(group == groups[i].astype(F32), every, 0.0)
                one = jnp.sum(jnp.sum(mine, axis=0, keepdims=True), axis=1, keepdims=True)
                two = jnp.sum(
                    jnp.sum(mine * mine, axis=0, keepdims=True), axis=1, keepdims=True
                )
                mean = jnp.where(lane1 == i, one / GSIZE, mean)
                square = jnp.where(lane1 == i, two / GSIZE, square)
            own = table[0:1]
            gained = (own - mean) * lax.rsqrt(square - mean * mean + 0.25)
    for trip in gc:
        trip[0].wait_recv()
        trip[2].start()
    for i in range(3):
        ec[i].wait_recv()
    total = jnp.sum(err[...] + ebuf[0] + ebuf[1] + ebuf[2], axis=1, keepdims=True)
    elane = lax.broadcasted_iota(jnp.int32, err.shape, 1)
    total = jnp.sum(jnp.where(erow == elane, total, 0.0), axis=0, keepdims=True)
    logp = -0.5 * total / (live * bt * c).astype(F32)
    fin[...] = jnp.where(frow == 0, logp, gained)
    place.wait()
    for trip in gc:
        trip[1].wait_recv()
        trip[2].wait_recv()

    for r in range(out.shape[0]):
        out[r] = blocks[pos_s[0, r]]
    for cp in ic:
        cp.wait_send()
    for q in range(nblk):

        @pl.when(q // jm != me)
        def _():
            sending(q).wait_send()

    for trip in gc:
        for cp in trip:
            cp.wait_send()
    for i in range(3):
        hc[i].wait_send()
        wc[i].wait_send()
        ec[i].wait_send()


def local(
    frames, owners, offsets, groups, latent, noise_blocks, rewards,
    embed_weight, norm_gain, mid_weight, head_weight,
):
    spd = frames.shape[0]
    devices = lax.axis_size("dp")
    mp = lax.axis_size("mp")
    nslot, c, bt = latent.shape
    width = embed_weight.shape[1]
    hidden = mid_weight.shape[1]
    pair_cap = (nslot + devices - 1) // devices
    jm = (pair_cap + mp - 1) // mp
    cap = jm * mp
    bpc = 2 if devices * jm % 2 == 0 else 1
    nchunk = devices * jm // bpc
    dims = (devices, mp, jm, bpc)
    rows8 = (spd + 7) // 8 * 8
    cap8 = (cap + 7) // 8 * 8
    steps = 4
    kc = width // steps
    smem = pl.BlockSpec(memory_space=pltpu.SMEM)
    vmem = pl.BlockSpec(memory_space=pltpu.VMEM)
    hbm = pl.BlockSpec(memory_space=pl.ANY)
    shape = jax.ShapeDtypeStruct
    dma = pltpu.SemaphoreType.DMA
    nblk = devices * jm
    prediction, fin = pl.pallas_call(
        functools.partial(main_kernel, dims),
        in_specs=[smem] * 5 + [vmem] * 3 + [hbm] * 3,
        out_specs=[vmem] * 2,
        out_shape=[shape((3 * spd, c, bt), BF16), shape((8, 128), F32)],
        scratch_shapes=[
            pltpu.VMEM((nslot, c, bt), BF16),
            pltpu.VMEM((nslot, c, bt), BF16),
            pltpu.VMEM((steps, kc, hidden), BF16),
            pltpu.VMEM((nchunk, c, bpc * bt), BF16),
            pltpu.VMEM((c, hidden), BF16),
            pltpu.VMEM((3, 2, c, hidden), BF16),
            pltpu.VMEM((hidden, c), BF16),
            pltpu.VMEM((nchunk, 1, bpc * bt), F32),
            pltpu.VMEM((nchunk, c, bpc * bt), F32),
            pltpu.VMEM((nblk, c, bt), BF16),
            pltpu.VMEM((mp * nblk, c, bt), BF16),
            pltpu.VMEM((rows8, bt), F32),
            pltpu.VMEM((3, rows8, bt), F32),
            pltpu.VMEM((cap8, 128), jnp.int32),
            pltpu.SMEM((cap8, 128), jnp.int32),
            pltpu.VMEM((cap8, 128), jnp.int32),
            pltpu.VMEM((devices, cap8, 128), jnp.int32),
            pltpu.VMEM((8, 128), F32),
            pltpu.VMEM((devices, 8, 128), F32),
            pltpu.VMEM((8, 128), jnp.int32),
            pltpu.SMEM((8, 128), jnp.int32),
            dma((3, 2)), dma((3, 2)),
            dma((2, devices)), dma((2, devices)),
            dma((nblk,)), dma((nblk,)),
            dma((3, nblk)), dma((3, nblk)),
            dma((3,)), dma((3,)),
            dma((2,)), dma((steps + 2,)),
        ],
        compiler_params=pltpu.CompilerParams(collective_id=0, has_side_effects=True),
        name="regroup",
    )(
        frames, owners, offsets, groups, rewards,
        embed_weight, norm_gain.reshape(1, width), head_weight.T,
        latent, noise_blocks, mid_weight,
    )
    return (prediction, fin[0, :spd], fin[1, :spd])


def solution(mesh):
    placed = (
        P("dp"),
        P("dp"),
        P("dp"),
        P("dp"),
        P("dp", None, None),
        P("dp", None, None),
        P("dp"),
        P(),
        P(),
        P(None, "mp"),
        P("mp", None),
    )
    return jax.shard_map(
        local,
        mesh=mesh,
        in_specs=placed,
        out_specs=(P("dp", None, None), P("dp"), P("dp")),
        check_vma=False,
    )
```

```python
import functools

import jax
import jax.numpy as jnp
from jax import lax
from jax.experimental import pallas as pl
from jax.experimental.pallas import tpu as pltpu
from jax.sharding import PartitionSpec as P

MAXB = 5
GSIZE = 12
F32 = jnp.float32
BF16 = jnp.bfloat16


def main_kernel(
    dims, frames, owners, offsets, groups, rewards, embed, gain, head, latent, noise, mid,
    out, fin,
    lat, noi, mids, tokens, wown, wbuf, wt, half, vel, pred, blocks, err, ebuf,
    slot_v, slot_s, ints, intr, flts, fltr, pos_v, pos_s,
    wsend, wrecv, isend, irecv, psend, precv, gsend, grecv, esend, erecv, local_sem, load_sem,
):
    devices, mp, jm, bpc = dims
    cap = jm * mp
    c, width = embed.shape
    bt = latent.shape[2]
    nslot = owners.shape[0]
    spd = frames.shape[0]
    nchunk = tokens.shape[0]
    nblk = devices * jm
    steps, kc, _ = mids.shape
    short = nchunk <= 4
    loads = [pltpu.make_async_copy(latent, lat, load_sem.at[0])]
    for i in range(steps):
        loads.append(
            pltpu.make_async_copy(mid.at[pl.ds(i * kc, kc)], mids.at[i], load_sem.at[1 + i])
        )
    loads.append(pltpu.make_async_copy(noise, noi, load_sem.at[1 + steps]))
    for cp in loads:
        cp.start()
    me = lax.axis_index("dp")
    m = lax.axis_index("mp")
    partner = m + 1 - 2 * (m % 2)
    across = (m + 2) % 4
    diag = (partner + 2) % 4

    def copy(src, dst, ssem, rsem, dp, mp):
        return pltpu.make_async_remote_copy(
            src_ref=src, dst_ref=dst, send_sem=ssem, recv_sem=rsem,
            device_id=(dp, mp), device_id_type=pl.DeviceIdType.MESH,
        )

    barrier = pltpu.get_barrier_semaphore()
    for p in (partner, across, diag):
        pl.semaphore_signal(
            barrier, inc=1, device_id=(me, p), device_id_type=pl.DeviceIdType.MESH
        )
    for d in range(1, devices):
        pl.semaphore_signal(
            barrier, inc=1, device_id=((me + d) % devices, m),
            device_id_type=pl.DeviceIdType.MESH,
        )

    row = lax.broadcasted_iota(jnp.int32, slot_v.shape, 0)
    lane = lax.broadcasted_iota(jnp.int32, slot_v.shape, 1)
    slot_of = jnp.full(slot_v.shape, -1, jnp.int32)
    row_of = slot_of
    seen = jnp.zeros(slot_v.shape, jnp.int32)
    live = jnp.ones((1, 128), jnp.int32)
    lane1 = lax.broadcasted_iota(jnp.int32, (1, 128), 1)
    for i in range(nslot):
        if i % MAXB == 0:
            blocks_here = lax.shift_right_arithmetic(frames[i // MAXB] - 1, 5) + 1
            live = jnp.where(lane1 == i // MAXB, blocks_here, live)
        hit = lane == jnp.where(i % MAXB < blocks_here, owners[i], -1)
        new = hit & (seen == row)
        slot_of = jnp.where(new, i, slot_of)
        row_of = jnp.where(new, offsets[i], row_of)
        seen = jnp.where(hit, seen + 1, seen)
    slot_v[...] = slot_of
    ints[...] = row_of
    frow = lax.broadcasted_iota(jnp.int32, (8, 128), 0)
    flane = lax.broadcasted_iota(jnp.int32, (8, 128), 1)
    table = jnp.full((8, 128), -1.0, F32)
    for i in range(spd):
        table = jnp.where((frow == 0) & (flane == i), rewards[i], table)
        table = jnp.where((frow == 1) & (flane == i), groups[i].astype(F32), table)
    flts[...] = table
    to_smem = pltpu.make_async_copy(slot_v, slot_s, local_sem.at[0])
    to_smem.start()
    w = embed[...]
    gram = lax.dot_general(w, w, (((1,), (1,)), ((), ())), preferred_element_type=F32)
    pl.semaphore_wait(barrier, 3 + devices - 1)

    def trio(src, part):
        return [
            copy(src, wbuf.at[0, part], wsend.at[0, part], wrecv.at[0, part], me, partner),
            copy(src, wbuf.at[1, part], wsend.at[1, part], wrecv.at[1, part], me, across),
            copy(
                wbuf.at[1, part], wbuf.at[2, part], wsend.at[2, part], wrecv.at[2, part],
                me, partner,
            ),
        ]

    hc = trio(head, 1)
    wc = trio(wown, 0)
    hc[1].start()
    hc[0].start()
    ic = []
    for d in range(1, devices):
        peer = (me + d) % devices
        ic.append(copy(ints, intr.at[me], isend.at[0, d], irecv.at[0, d], peer, m))
        ic.append(copy(flts, fltr.at[me], isend.at[1, d], irecv.at[1, d], peer, m))
    for cp in ic:
        cp.start()
    intr[me] = row_of
    fltr[me] = table

    to_smem.wait()
    loads[0].wait()

    def prepare(k, z):
        for b in range(bpc):
            q = k * bpc + b
            s = jnp.maximum(slot_s[m * jm + q % jm, q // jm], 0)
            tokens[k, :, b * bt : (b + 1) * bt] = lat[s]
        x = tokens[k].astype(F32)
        y = jnp.dot(gram, x, preferred_element_type=F32, precision=lax.Precision.HIGHEST)
        ms = jnp.maximum(jnp.sum(x * y, axis=0, keepdims=True), 0.0) / width
        half[k] = 0.5 * lax.rsqrt(ms + 0.25)
        return z

    lax.fori_loop(0, nchunk, prepare, 0, unroll=short)

    folded = None
    for i in range(steps):
        wg = embed[:, i * kc : (i + 1) * kc].astype(F32) * gain[:, i * kc : (i + 1) * kc]
        hi = wg.astype(BF16)
        lo = (wg - hi.astype(F32)).astype(BF16)
        loads[1 + i].wait()
        both = jnp.dot(
            jnp.concatenate([hi, lo], axis=0), mids[i], preferred_element_type=F32
        )
        folded = both if i == 0 else folded + both
    folded = folded[:c] + folded[c:]
    wown[...] = folded.astype(BF16)
    wt[...] = folded.T.astype(BF16)
    wc[1].start()
    wc[0].start()
    hc[1].wait_recv()
    hc[2].start()

    def part(href, k):
        u = jnp.dot(wt[...], tokens[k], preferred_element_type=F32)
        h = u * half[k]
        act = (h + h * jnp.tanh(h)).astype(BF16)
        return jnp.dot(href[...], act, preferred_element_type=F32)

    def share(href, first):
        def body(k, z):
            v = part(href, k)
            vel[k] = v if first else vel[k] + v
            return z

        lax.fori_loop(0, nchunk, body, 0, unroll=short)

    share(head, True)
    hc[0].wait_recv()
    wc[0].wait_recv()
    wt[...] = wbuf[0, 0].astype(F32).T.astype(BF16)
    share(wbuf.at[0, 1], False)
    wc[1].wait_recv()
    wc[2].start()
    wt[...] = wbuf[1, 0].astype(F32).T.astype(BF16)
    share(wbuf.at[1, 1], False)
    hc[2].wait_recv()
    wc[2].wait_recv()
    wt[...] = wbuf[2, 0].astype(F32).T.astype(BF16)
    err[...] = jnp.zeros_like(err)
    erow = lax.broadcasted_iota(jnp.int32, err.shape, 0)
    loads[1 + steps].wait()

    def sending(q):
        o, jj = q // jm, q % jm
        return copy(
            pred.at[q], blocks.at[(m * devices + me) * jm + jj],
            psend.at[q], precv.at[me * jm + jj], o, m,
        )

    def keeping(q):
        return pltpu.make_async_copy(
            pred.at[q], blocks.at[(m * devices + me) * jm + q % jm], psend.at[q]
        )

    def last(step, z):
        k = (me * jm // bpc + 1 + step) % nchunk
        v = vel[k] + part(wbuf.at[2, 1], k)
        for b in range(bpc):
            q = k * bpc + b
            vb = v[:, b * bt : (b + 1) * bt]
            pred[q] = vb.astype(BF16)

            @pl.when(q // jm != me)
            def _():
                sending(q).start()

            @pl.when(q // jm == me)
            def _():
                keeping(q).start()

            s = slot_s[m * jm + q % jm, q // jm]
            e = noi[jnp.maximum(s, 0)].astype(F32) + vb
            e = jnp.sum(e * e, axis=0, keepdims=True)
            sample = jnp.where(s < 0, -1, s // MAXB)
            err[...] += jnp.where(erow == sample, e, 0.0)
        return z

    lax.fori_loop(0, nchunk, last, 0, unroll=short)
    ec = []
    for i, p in enumerate((partner, across, diag)):
        cp = copy(err, ebuf.at[i], esend.at[i], erecv.at[i], me, p)
        cp.start()
        ec.append(cp)

    def moves(n, src, jj):
        at = blocks.at[(m * devices + src) * jm + jj]
        far = blocks.at[(across * devices + src) * jm + jj]
        return (
            copy(at, at, gsend.at[0, n], grecv.at[0, n], me, across),
            copy(at, at, gsend.at[1, n], grecv.at[1, n], me, partner),
            copy(far, far, gsend.at[2, n], grecv.at[2, n], me, partner),
        )

    gc = []
    for d in range(devices):
        src = (me - d + devices) % devices
        for jj in range(jm):
            trip = moves(d * jm + jj, src, jj)
            gc.append(trip)
            if d == 0:
                keeping(me * jm + jj).wait()
            else:
                pltpu.make_async_remote_copy(
                    src_ref=pred.at[0], dst_ref=blocks.at[(m * devices + src) * jm + jj],
                    send_sem=psend.at[0], recv_sem=precv.at[src * jm + jj],
                    device_id=(src, m), device_id_type=pl.DeviceIdType.MESH,
                ).wait_recv()
            trip[0].start()
            trip[1].start()
        if d == 0:
            for cp in ic:
                cp.wait_recv()
            code = jnp.full(slot_v.shape, -1, jnp.int32)
            for j in range(cap):
                code = jnp.where(row == j, (j // jm * devices) * jm + j % jm, code)
            pos = jnp.zeros(slot_v.shape, jnp.int32)
            mean = jnp.zeros((1, 128), F32)
            square = jnp.zeros((1, 128), F32)
            for s in range(devices):
                want = jnp.max(
                    jnp.where((lane == me) & (row < cap), intr[s], -1), axis=1, keepdims=True
                )
                pos = jnp.maximum(pos, jnp.where(want == lane, code + s * jm, 0))
            pos_v[...] = jnp.broadcast_to(jnp.max(pos, axis=0, keepdims=True), pos_v.shape)
            place = pltpu.make_async_copy(pos_v, pos_s, local_sem.at[1])
            place.start()
            every = fltr[:, 0, :]
            group = fltr[:, 1, :]
            for i in range(spd):
                mine = jnp.where(group == groups[i].astype(F32), every, 0.0)
                one = jnp.sum(jnp.sum(mine, axis=0, keepdims=True), axis=1, keepdims=True)
                two = jnp.sum(
                    jnp.sum(mine * mine, axis=0, keepdims=True), axis=1, keepdims=True
                )
                mean = jnp.where(lane1 == i, one / GSIZE, mean)
                square = jnp.where(lane1 == i, two / GSIZE, square)
            own = table[0:1]
            gained = (own - mean) * lax.rsqrt(square - mean * mean + 0.25)
    for trip in gc:
        trip[0].wait_recv()
        trip[2].start()
    for i in range(3):
        ec[i].wait_recv()
    total = jnp.sum(err[...] + ebuf[0] + ebuf[1] + ebuf[2], axis=1, keepdims=True)
    elane = lax.broadcasted_iota(jnp.int32, err.shape, 1)
    total = jnp.sum(jnp.where(erow == elane, total, 0.0), axis=0, keepdims=True)
    logp = -0.5 * total / (live * bt * c).astype(F32)
    fin[...] = jnp.where(frow == 0, logp, gained)
    place.wait()
    for trip in gc:
        trip[1].wait_recv()
        trip[2].wait_recv()

    for r in range(out.shape[0]):
        out[r] = blocks[pos_s[0, r]]
    for cp in ic:
        cp.wait_send()
    for q in range(nblk):

        @pl.when(q // jm != me)
        def _():
            sending(q).wait_send()

    for trip in gc:
        for cp in trip:
            cp.wait_send()
    for i in range(3):
        hc[i].wait_send()
        wc[i].wait_send()
        ec[i].wait_send()


def finish_kernel(fin, rows, out, logp, gained):
    out[...] = rows[...]
    for i in range(logp.shape[0]):
        logp[i] = fin[0, i]
        gained[i] = fin[1, i]


def local(
    frames, owners, offsets, groups, latent, noise_blocks, rewards,
    embed_weight, norm_gain, mid_weight, head_weight,
):
    spd = frames.shape[0]
    devices = lax.axis_size("dp")
    mp = lax.axis_size("mp")
    nslot, c, bt = latent.shape
    width = embed_weight.shape[1]
    hidden = mid_weight.shape[1]
    pair_cap = (nslot + devices - 1) // devices
    jm = (pair_cap + mp - 1) // mp
    cap = jm * mp
    bpc = 4 if devices * jm % 4 == 0 else 1
    nchunk = devices * jm // bpc
    dims = (devices, mp, jm, bpc)
    rows8 = (spd + 7) // 8 * 8
    cap8 = (cap + 7) // 8 * 8
    steps = 4
    kc = width // steps
    smem = pl.BlockSpec(memory_space=pltpu.SMEM)
    vmem = pl.BlockSpec(memory_space=pltpu.VMEM)
    hbm = pl.BlockSpec(memory_space=pl.ANY)
    shape = jax.ShapeDtypeStruct
    dma = pltpu.SemaphoreType.DMA
    nblk = devices * jm
    placed_rows, fin = pl.pallas_call(
        functools.partial(main_kernel, dims),
        in_specs=[smem] * 5 + [vmem] * 3 + [hbm] * 3,
        out_specs=[vmem] * 2,
        out_shape=[shape((3 * spd, c, bt), BF16), shape((8, 128), F32)],
        scratch_shapes=[
            pltpu.VMEM((nslot, c, bt), BF16),
            pltpu.VMEM((nslot, c, bt), BF16),
            pltpu.VMEM((steps, kc, hidden), BF16),
            pltpu.VMEM((nchunk, c, bpc * bt), BF16),
            pltpu.VMEM((c, hidden), BF16),
            pltpu.VMEM((3, 2, c, hidden), BF16),
            pltpu.VMEM((hidden, c), BF16),
            pltpu.VMEM((nchunk, 1, bpc * bt), F32),
            pltpu.VMEM((nchunk, c, bpc * bt), F32),
            pltpu.VMEM((nblk, c, bt), BF16),
            pltpu.VMEM((mp * nblk, c, bt), BF16),
            pltpu.VMEM((rows8, bt), F32),
            pltpu.VMEM((3, rows8, bt), F32),
            pltpu.VMEM((cap8, 128), jnp.int32),
            pltpu.SMEM((cap8, 128), jnp.int32),
            pltpu.VMEM((cap8, 128), jnp.int32),
            pltpu.VMEM((devices, cap8, 128), jnp.int32),
            pltpu.VMEM((8, 128), F32),
            pltpu.VMEM((devices, 8, 128), F32),
            pltpu.VMEM((8, 128), jnp.int32),
            pltpu.SMEM((8, 128), jnp.int32),
            dma((3, 2)), dma((3, 2)),
            dma((2, devices)), dma((2, devices)),
            dma((nblk,)), dma((nblk,)),
            dma((3, nblk)), dma((3, nblk)),
            dma((3,)), dma((3,)),
            dma((2,)), dma((steps + 2,)),
        ],
        compiler_params=pltpu.CompilerParams(collective_id=0, has_side_effects=True),
        name="regroup",
    )(
        frames, owners, offsets, groups, rewards,
        embed_weight, norm_gain.reshape(1, width), head_weight.T,
        latent, noise_blocks, mid_weight,
    )
    return pl.pallas_call(
        finish_kernel,
        in_specs=[smem, vmem],
        out_specs=[vmem, smem, smem],
        out_shape=[shape((3 * spd, c, bt), BF16), shape((spd,), F32), shape((spd,), F32)],
        name="finish",
    )(fin, placed_rows)


def solution(mesh):
    placed = (
        P("dp"),
        P("dp"),
        P("dp"),
        P("dp"),
        P("dp", None, None),
        P("dp", None, None),
        P("dp"),
        P(),
        P(),
        P(None, "mp"),
        P("mp", None),
    )
    return jax.shard_map(
        local,
        mesh=mesh,
        in_specs=placed,
        out_specs=(P("dp", None, None), P("dp"), P("dp")),
        check_vma=False,
    )
```
